256 devices in a mesh: groups: 2 (over z), ep: 128 (over y, x, core).
Axes of the slice: x: 8, y: 8, z: 2, core: 2. Of those that a mesh axis runs over, the one named last changes fastest.
The devices are a block of a 8x8x16 slice.
Arguments:
- tokens: bfloat16 [2048, 2880], P(('groups', 'ep')), parts along dimension 0, may hold values from -6 to 6
- norm_gain: float32 [2880], replicated, may hold values from 0.1 to 1.9
- expert_ids: int32 [2048, 4], P(('groups', 'ep')), parts along dimension 0, may hold values from 0 to 63, all different within a row; in each aligned block of 8 rows (0 to 7, 8 to 15, ...) at most 1 rows name the same one
- gate_codes: int32 [2048, 4], P(('groups', 'ep')), parts along dimension 0, may hold values from 1 to 65535
- w_gate: bfloat16 [128, 2880, 720], P('ep'), may hold values from -0.109375 to 0.109375
- w_up: bfloat16 [128, 2880, 720], P('ep'), may hold values from -0.109375 to 0.109375
- w_down: bfloat16 [128, 720, 2880], P('ep'), may hold values from -0.15625 to 0.15625
Outputs:
- updated: bfloat16 [2048, 2880], P(('groups', 'ep')), parts along dimension 0
The draws below stay inside these ranges and needn't reach their ends.
There are 2 independent parts, one for each index of `groups`. The reference program is written for one: setup_inputs(seed, part) draws one part's arguments, and reference() takes and returns one part's arrays. A program takes and returns all parts, laid end to end along the dimension named above; an argument that names none is the same for every part. Nothing has to cross between parts.
Inputs may be any that keep to these rules, and one draw needn't show every extreme that they name: `expert_ids`: each token names 4 different experts. Among the tokens of one device (aligned blocks of 8 rows) no expert is named more than once, and in every draw some expert is named exactly once by some device's tokens.
All inputs are finite; a program needn't handle non-finite values.
Results may differ from the reference program's by a relative error of at most 0.0049.
Values may be sent and summed in bfloat16 or wider, within the bound.
No kernel may reach another device: no remote copies, remote signals or barrier semaphores. Data moves between devices by JAX's collectives and lax.ppermute only.
A program may use at most 64 MiB of HBM per device.

```python
import math
import jax
import jax.numpy as jnp
import numpy as np
from jax import lax

D = 2880
FF = 1440
TOP = 4
HALVES = 2
TOK_DEV = 8
EXPERTS = 64
SHARD_FF = 720
CAP = 1
TOKENS = 1024
N_EP = 128


def plant(entries, stream_key, smallest, high):
    place = [jax.random.randint(jax.random.fold_in(stream_key, axis), (), 0, length) for axis, length in enumerate(entries.shape)]
    main_axis = entries.shape.index(max(entries.shape))
    beside = place[:main_axis] + [(place[main_axis] + 1) % entries.shape[main_axis]] + place[main_axis + 1:]
    return entries.at[tuple(place)].set(smallest).at[tuple(beside)].set(high)


def block_levels(key, shape, split, low, high):
    def one(position, shards_of):
        steps = jax.random.uniform(jax.random.fold_in(jax.random.fold_in(key, 6), position), (shards_of,), jnp.float32, low / len(split), high / len(split))
        return jnp.repeat(jnp.exp(steps), shape[position] // shards_of).reshape((-1,) + (1,) * (len(shape) - position - 1))

    factor_of = one(*split[0])
    for cut in split[1:]:
        factor_of = factor_of * one(*cut)
    return factor_of


def assign_block(stream_key, own, number, rows, count, top, bound, skew):
    sequence = jax.random.permutation(stream_key, count)
    packed, usual = load_shares(count, rows * top, bound, skew, True), load_shares(count, rows * top, bound, skew, False)
    places = jnp.arange(count)

    def named(sizes, turn):
        used = int((sizes > 0).sum())
        fixed = max(1, used // 4)
        moved = fixed + (places - fixed + turn * (used - fixed)) % max(1, count - fixed)
        return jnp.zeros((count,), jnp.int32).at[sequence[jnp.where(places < fixed, places, moved)]].set(jnp.asarray(sizes, jnp.int32))

    sizes = jnp.where(number % 4 == 0, named(packed, number // 4), named(usual, number - number // 4 - 1))
    mixed = jax.random.permutation(jax.random.fold_in(own, 3), count)
    source_of, taker = mixed[0:count // 2 * 2:2], mixed[1:count // 2 * 2:2]
    slack = jnp.minimum(sizes[source_of] - 1, bound - sizes[taker]) // 2
    slack = jnp.where((source_of == sequence[0]) | (taker == sequence[0]) | (sizes[taker] == 0), 0, jnp.maximum(slack, 0))
    moved = jax.random.randint(jax.random.fold_in(own, 4), (count // 2,), 0, 1 << 20) % (slack + 1)
    sizes = sizes.at[source_of].add(-moved).at[taker].add(moved)
    labels = jnp.searchsorted(jnp.cumsum(sizes), jnp.arange(rows * top), side="right").astype(jnp.int32)
    table = labels.reshape(top, rows).T
    table = table[jax.random.permutation(jax.random.fold_in(own, 1), rows)]
    turn = jax.random.randint(jax.random.fold_in(own, 2), (rows, 1), 0, top)
    return jnp.take_along_axis(table, (jnp.arange(top)[None, :] + turn) % top, axis=1)


def load_shares(number_of, total, most, slope, full):
    weights = [(1 << 20) // math.isqrt(rank ** slope) + 1 for rank in range(1, number_of + 1)]
    largest = most if full else min(most, max(-(-total // number_of), total * weights[0] // sum(weights)))
    least = 1 if total - largest >= number_of - 1 else 0
    holding, rest = [largest] + [least] * (number_of - 1), total - largest - least * (number_of - 1)
    while rest > 0:
        movable = [i for i in range(1, number_of) if holding[i] < largest] or [i for i in range(1, number_of) if holding[i] < most]
        whole, left = sum([weights[i] for i in movable]), rest
        for i in movable:
            extra = min(most - holding[i], max(1, left * weights[i] // whole), rest)
            holding[i] = holding[i] + extra
            rest = rest - extra
    return np.array(holding)


def noise(key, shape, scale, bound, split=(), kind=jnp.bfloat16):
    drawn = jax.random.normal(key, shape, jnp.float32) * scale
    if len(split) > 0:
        drawn = block_levels(key, shape, split, -0.22, 0.18) * drawn
    return jnp.clip(drawn, min=-bound, max=bound).astype(kind)


def setup_inputs(seed: int = 0, part: int = 0) -> dict:
    arg_keys = jax.random.split(jax.random.key(seed), 8)
    part_splits = jax.random.split(jax.random.fold_in(arg_keys[7], part), 8)
    tokens = noise(part_splits[0], (TOKENS, D), 1.0, 6.0, ((0, 128),))
    norm_gain = jnp.clip(1.0 + 0.18 * jax.random.normal(arg_keys[1], (D,), jnp.float32), 0.1, 1.9)
    expert_ids_keys = jax.random.split(jax.random.fold_in(part_splits[2], 1), TOKENS // TOK_DEV)
    expert_ids_turns = jax.random.permutation(jax.random.fold_in(part_splits[2], 3), TOKENS // TOK_DEV)
    expert_ids = jax.vmap(lambda own, number: assign_block(jax.random.fold_in(part_splits[2], 2), own, number, TOK_DEV, EXPERTS, TOP, CAP, 2))(expert_ids_keys, expert_ids_turns).reshape((TOKENS, TOP))
    gate_codes = plant(jax.random.randint(part_splits[3], (TOKENS, TOP), 1, 65536), jax.random.fold_in(part_splits[3], 1), 1, 65535).astype(jnp.int32)
    w_gate = noise(arg_keys[4], (EXPERTS * HALVES, D, SHARD_FF), D ** -0.5, 0.109375, ((0, 128),))
    w_up = noise(arg_keys[5], (EXPERTS * HALVES, D, SHARD_FF), D ** -0.5, 0.109375, ((0, 128),))
    w_down = noise(arg_keys[6], (EXPERTS * HALVES, SHARD_FF, D), FF ** -0.5, 0.15625, ((0, 128),))
    return dict(tokens=tokens, norm_gain=norm_gain, expert_ids=expert_ids, gate_codes=gate_codes, w_gate=w_gate, w_up=w_up, w_down=w_down)


epsilon = 1e-05

def reference(tokens, norm_gain, expert_ids, gate_codes, w_gate, w_up, w_down):
    values = tokens.astype(jnp.float32)
    normed = (values * lax.rsqrt(lax.optimization_barrier(jnp.mean(values * values, axis=1, keepdims=True)) + epsilon) * norm_gain).astype(jnp.bfloat16)
    code_values = gate_codes.astype(jnp.float32)
    weights = code_values / lax.optimization_barrier(jnp.sum(code_values, axis=1, keepdims=True))
    pair_total = TOKENS * TOP
    room = N_EP * CAP
    flat_ids = expert_ids.reshape(-1).astype(jnp.int32)
    gates_all = w_gate.reshape(EXPERTS, HALVES, D, SHARD_FF)
    ups_all = w_up.reshape(EXPERTS, HALVES, D, SHARD_FF)
    downs_all = w_down.reshape(EXPERTS, HALVES, SHARD_FF, D)

    def one_expert(expert, per_pair):
        indices = jnp.nonzero(flat_ids == expert, size=room, fill_value=pair_total)[0].astype(jnp.int32)
        token_rows = normed[jnp.minimum(indices, pair_total - 1) // TOP].astype(jnp.float32)
        gate_mat = lax.dynamic_index_in_dim(gates_all, expert, 0, keepdims=False)
        gate_mat = jnp.transpose(gate_mat, (1, 0, 2)).reshape(D, FF).astype(jnp.float32)
        up_mat = lax.dynamic_index_in_dim(ups_all, expert, 0, keepdims=False)
        up_mat = jnp.transpose(up_mat, (1, 0, 2)).reshape(D, FF).astype(jnp.float32)
        down_mat = lax.dynamic_index_in_dim(downs_all, expert, 0, keepdims=False).astype(jnp.float32)
        gate_out = jnp.dot(token_rows, gate_mat, precision=lax.Precision.HIGHEST, preferred_element_type=jnp.float32)
        upward = jnp.dot(token_rows, up_mat, precision=lax.Precision.HIGHEST, preferred_element_type=jnp.float32)
        hidden = (jax.nn.silu(gate_out) * upward).astype(jnp.bfloat16).astype(jnp.float32)
        share_low = jnp.dot(hidden[:, :SHARD_FF], down_mat[0], precision=lax.Precision.HIGHEST, preferred_element_type=jnp.float32).astype(jnp.bfloat16)
        share_high = jnp.dot(hidden[:, SHARD_FF:], down_mat[1], precision=lax.Precision.HIGHEST, preferred_element_type=jnp.float32).astype(jnp.bfloat16)
        output = (share_low.astype(jnp.float32) + share_high.astype(jnp.float32)).astype(jnp.bfloat16)
        return per_pair.at[indices].set(output, mode='drop')
    per_pair = lax.fori_loop(0, EXPERTS, one_expert, jnp.zeros((pair_total, D), jnp.bfloat16))
    mixture = lax.optimization_barrier(jnp.sum(per_pair.reshape(TOKENS, TOP, D).astype(jnp.float32) * weights[:, :, None], axis=1))
    return (values + mixture).astype(jnp.bfloat16)
```

```python
import functools

import jax
import jax.numpy as jnp
from jax import lax
from jax.experimental import pallas as pl
from jax.experimental.pallas import tpu as pltpu
from jax.sharding import PartitionSpec as P

epsilon = 1e-05
PIECES = 8
NT = (((1,), (1,)), ((), ()))


def piece_width(model_width):
    return -(-model_width // (PIECES * 128)) * 128


def stack_pieces(rows, width):
    d = rows.shape[1]
    parts = []
    for s in range(PIECES):
        part = rows[:, s * width : min((s + 1) * width, d)]
        if part.shape[1] < width:
            part = jnp.concatenate(
                [part, jnp.zeros((rows.shape[0], width - part.shape[1]), rows.dtype)], axis=1
            )
        parts.append(part)
    return jnp.concatenate(parts, axis=0)


def swap_matrix(outer, inner):
    total = outer * inner
    row = lax.broadcasted_iota(jnp.int32, (total, total), 0)
    col = lax.broadcasted_iota(jnp.int32, (total, total), 1)
    source = (row % inner) * outer + row // inner
    return jnp.where(col == source, 1.0, 0.0).astype(jnp.bfloat16)


def route_kernel(tokens_ref, gain_ref, ids_ref, out_ref, *, experts, width):
    values = tokens_ref[...].astype(jnp.float32)
    count = values.shape[0]
    scale = lax.rsqrt(jnp.mean(values * values, axis=1, keepdims=True) + epsilon)
    normed = values * scale * gain_ref[...]
    stacked = stack_pieces(normed, width).astype(jnp.bfloat16)
    ids = ids_ref[...].astype(jnp.float32)
    top = ids.shape[0]
    columns = PIECES * count
    spread = jnp.where(
        lax.broadcasted_iota(jnp.int32, (count, columns), 1) % count
        == lax.broadcasted_iota(jnp.int32, (count, columns), 0),
        1.0,
        0.0,
    )
    ids_wide = jnp.dot(
        ids.astype(jnp.bfloat16), spread.astype(jnp.bfloat16), preferred_element_type=jnp.float32
    ).astype(jnp.int32)
    piece = lax.broadcasted_iota(jnp.int32, (top, columns), 1) // count
    wanted = ids_wide * PIECES + piece
    row = lax.broadcasted_iota(jnp.int32, (experts * PIECES, columns), 0)
    hit = row == wanted[0:1, :]
    for k in range(1, top):
        hit = jnp.logical_or(hit, row == wanted[k : k + 1, :])
    placing = jnp.where(hit, 1.0, 0.0).astype(jnp.bfloat16)
    out_ref[...] = jnp.dot(placing, stacked, preferred_element_type=jnp.float32).astype(
        jnp.bfloat16
    )


def expert_kernel(own_ref, other_ref, gate_ref, up_ref, down_ref, own_out, other_out, *, width):
    rows = own_ref.shape[0] // PIECES
    model = gate_ref.shape[1]
    swap = swap_matrix(PIECES, rows)
    halves = []
    for ref in (own_ref, other_ref):
        moved = jnp.dot(swap, ref[...], preferred_element_type=jnp.float32).astype(jnp.bfloat16)
        halves.append(
            jnp.concatenate([moved[s * rows : (s + 1) * rows] for s in range(PIECES)], axis=1)
        )
    x = jnp.concatenate(halves, axis=0)[:, :model]
    gate = lax.dot_general(gate_ref[...], x, NT, preferred_element_type=jnp.float32)
    up = lax.dot_general(up_ref[...], x, NT, preferred_element_type=jnp.float32)
    hidden = (gate * jax.nn.sigmoid(gate) * up).T.astype(jnp.bfloat16)
    out = jnp.dot(hidden, down_ref[...], preferred_element_type=jnp.float32).astype(jnp.bfloat16)
    own_out[...] = out[:rows]
    other_out[...] = out[rows:]


def add_kernel(own_ref, arrived_ref, out_ref, *, width):
    rows = own_ref.shape[0]
    total = own_ref[...].astype(jnp.float32) + arrived_ref[...].astype(jnp.float32)
    stacked = stack_pieces(total, width).astype(jnp.bfloat16)
    out_ref[...] = jnp.dot(
        swap_matrix(rows, PIECES), stacked, preferred_element_type=jnp.float32
    ).astype(jnp.bfloat16)


def combine_kernel(tokens_ref, ids_ref, codes_ref, returned_ref, out_ref, *, width):
    ids = ids_ref[...].T
    codes = codes_ref[...].astype(jnp.float32)
    weights = (codes / jnp.sum(codes, axis=0, keepdims=True)).T
    count, top = ids.shape
    rows = PIECES * count
    slots = returned_ref.shape[0]
    piece = lax.broadcasted_iota(jnp.int32, (rows, 1), 0) // count
    col = lax.broadcasted_iota(jnp.int32, (rows, slots), 1)
    mixture = None
    for k in range(top):
        wanted = jnp.concatenate([ids[:, k : k + 1]] * PIECES, axis=0) * PIECES + piece
        taking = jnp.where(col == wanted, 1.0, 0.0).astype(jnp.bfloat16)
        picked = jnp.dot(taking, returned_ref[...], preferred_element_type=jnp.float32)
        term = picked * jnp.concatenate([weights[:, k : k + 1]] * PIECES, axis=0)
        mixture = term if mixture is None else mixture + term
    model = tokens_ref.shape[1]
    for s in range(PIECES):
        span = min((s + 1) * width, model) - s * width
        here = pl.ds(s * width, span)
        out_ref[:, here] = (
            tokens_ref[:, here].astype(jnp.float32)
            + mixture[s * count : (s + 1) * count, :span]
        ).astype(jnp.bfloat16)


VMEM = pl.BlockSpec(memory_space=pltpu.VMEM)


def call(kernel, out_shape, limit, cost, *args):
    many = isinstance(out_shape, tuple)
    return pl.pallas_call(
        kernel,
        out_shape=out_shape,
        in_specs=[VMEM] * len(args),
        out_specs=(VMEM,) * len(out_shape) if many else VMEM,
        compiler_params=pltpu.CompilerParams(vmem_limit_bytes=limit),
        cost_estimate=pl.CostEstimate(flops=cost, bytes_accessed=0, transcendentals=0),
    )(*args)


def shards(tokens, norm_gain, expert_ids, gate_codes, w_gate, w_up, w_down):
    devices = lax.axis_size("ep")
    experts = devices // 2
    count, model = tokens.shape
    width = piece_width(model)
    slots = experts * PIECES
    message = jax.ShapeDtypeStruct((slots, width), jnp.bfloat16)
    same_core = [[2 * i + c for i in range(experts)] for c in range(2)]
    partner = [(i, i ^ 1) for i in range(devices)]
    ids = expert_ids.T
    codes = gate_codes.T

    def exchange(rows):
        return lax.all_to_all(
            rows.reshape(experts, PIECES, width),
            "ep",
            split_axis=0,
            concat_axis=0,
            axis_index_groups=same_core,
            tiled=True,
        ).reshape(slots, width)

    outgoing = call(
        functools.partial(route_kernel, experts=experts, width=width),
        message,
        4 << 20,
        20_000_000_000,
        tokens,
        norm_gain.reshape(1, model),
        ids,
    )
    arrived = exchange(outgoing)
    other = lax.ppermute(arrived, "ep", partner)
    share = jax.ShapeDtypeStruct((experts, model), jnp.bfloat16)
    own_share, other_share = call(
        functools.partial(expert_kernel, width=width),
        (share, share),
        32 << 20,
        2_000_000_000,
        arrived,
        other,
        w_gate[0].T,
        w_up[0].T,
        w_down[0],
    )
    returned = exchange(
        call(
            functools.partial(add_kernel, width=width),
            message,
            8 << 20,
            1_000_000,
            own_share,
            lax.ppermute(other_share, "ep", partner),
        )
    )
    return call(
        functools.partial(combine_kernel, width=width),
        jax.ShapeDtypeStruct((count, model), jnp.bfloat16),
        8 << 20,
        1_000_000,
        tokens,
        ids,
        codes,
        returned,
    )


def solution(mesh):
    return jax.shard_map(
        shards,
        mesh=mesh,
        in_specs=(
            P(("groups", "ep"), None),
            P(),
            P(("groups", "ep"), None),
            P(("groups", "ep"), None),
            P("ep", None, None),
            P("ep", None, None),
            P("ep", None, None),
        ),
        out_specs=P(("groups", "ep"), None),
        check_vma=False,
    )
```

```python
import functools

import jax
import jax.numpy as jnp
from jax import lax
from jax.experimental import pallas as pl
from jax.experimental.pallas import tpu as pltpu
from jax.sharding import PartitionSpec as P

epsilon = 1e-05
PIECES = 8
BLOCK = 32
NT = (((1,), (1,)), ((), ()))
F32 = jnp.float32
BF16 = jnp.bfloat16


def iota(shape, axis):
    return lax.broadcasted_iota(jnp.int32, shape, axis)


def onehot(mask):
    return jnp.where(mask, 1.0, 0.0).astype(BF16)


def matmul(a, b):
    return jnp.dot(a, b, preferred_element_type=F32)


def piece_width(model_width):
    return -(-model_width // (PIECES * 128)) * 128


def stack_pieces(rows, width):
    n, d = rows.shape
    parts = []
    for s in range(PIECES):
        part = rows[:, s * width : min((s + 1) * width, d)]
        if part.shape[1] < width:
            part = jnp.concatenate(
                [part, jnp.zeros((n, width - part.shape[1]), rows.dtype)], axis=1
            )
        parts.append(part)
    return jnp.concatenate(parts, axis=0)


def swap_matrix(outer, inner):
    total = outer * inner
    row = iota((total, total), 0)
    col = iota((total, total), 1)
    return onehot(col == (row % inner) * outer + row // inner)


def rows_of(messages_ref):
    size = BLOCK * PIECES
    swap = swap_matrix(PIECES, BLOCK)
    blocks = []
    for b in range(messages_ref.shape[0] // size):
        moved = matmul(swap, messages_ref[b * size : (b + 1) * size, :]).astype(BF16)
        blocks.append(
            jnp.concatenate([moved[s * BLOCK : (s + 1) * BLOCK] for s in range(PIECES)], axis=1)
        )
    return jnp.concatenate(blocks, axis=0)


def messages_block(rows, width):
    return matmul(swap_matrix(BLOCK, PIECES), stack_pieces(rows, width))


def spread_kernel(spread_ref):
    count, columns = spread_ref.shape
    spread_ref[...] = onehot(iota((count, columns), 1) % count == iota((count, columns), 0))


def route_kernel(tokens_ref, gain_ref, ids_ref, spread_ref, out_ref, *, experts, width):
    top, count = ids_ref.shape
    columns = PIECES * count
    piece = iota((top, columns), 1) // count
    row = iota((experts * PIECES, columns), 0)
    ids = ids_ref[...].astype(F32).astype(BF16)
    wanted = matmul(ids, spread_ref[...]).astype(jnp.int32) * PIECES + piece
    hit = row == wanted[0:1, :]
    for k in range(1, top):
        hit = jnp.logical_or(hit, row == wanted[k : k + 1, :])
    placing = onehot(hit)
    values = tokens_ref[...].astype(F32)
    scale = lax.rsqrt(jnp.mean(values * values, axis=1, keepdims=True) + epsilon)
    normed = values * scale * gain_ref[...].reshape(1, -1)
    stacked = stack_pieces(normed, width).astype(BF16)
    out_ref[...] = matmul(placing, stacked).astype(BF16)


def tables_kernel(arrived_ref, ids_ref, codes_ref, own_rows, taking, weighing, *, model):
    own_rows[...] = rows_of(arrived_ref)[:, :model]
    ids = ids_ref[...].T
    codes = codes_ref[...].astype(F32)
    weights = (codes / jnp.sum(codes, axis=0, keepdims=True)).T
    count, top = ids.shape
    rows = PIECES * count
    piece = iota((rows, 1), 0) // count
    col = iota((rows, taking.shape[1]), 1)
    for k in range(top):
        here = pl.ds(k * rows, rows)
        wanted = jnp.concatenate([ids[:, k : k + 1]] * PIECES, axis=0) * PIECES + piece
        taking[here, :] = onehot(col == wanted)
        weight = jnp.concatenate([weights[:, k : k + 1]] * PIECES, axis=0)
        weighing[here, :] = jnp.broadcast_to(weight, (rows, weighing.shape[1]))


def expert_kernel(own_rows, other_ref, gate_ref, up_ref, down_ref, own_out, other_out):
    rows, model = own_rows.shape
    x = jnp.concatenate([own_rows[...], rows_of(other_ref)[:, :model]], axis=0)
    gate = lax.dot_general(gate_ref[...], x, NT, preferred_element_type=F32)
    up = lax.dot_general(up_ref[...], x, NT, preferred_element_type=F32)
    hidden = (gate * jax.nn.sigmoid(gate) * up).T.astype(BF16)
    out = matmul(hidden, down_ref[...]).astype(BF16)
    own_out[...] = out[:rows]
    other_out[...] = out[rows:]


def messages_kernel(rows_ref, out_ref, *, width):
    size = BLOCK * PIECES
    for b in range(rows_ref.shape[0] // BLOCK):
        rows = rows_ref[b * BLOCK : (b + 1) * BLOCK, :].astype(F32).astype(BF16)
        out_ref[b * size : (b + 1) * size, :] = messages_block(rows, width).astype(BF16)


def add_kernel(own_ref, arrived_ref, out_ref, *, width):
    size = BLOCK * PIECES
    for b in range(arrived_ref.shape[0] // BLOCK):
        here = pl.ds(b * size, size)
        moved = messages_block(arrived_ref[b * BLOCK : (b + 1) * BLOCK, :], width)
        out_ref[here, :] = (own_ref[here, :].astype(F32) + moved).astype(BF16)


def combine_kernel(tokens_ref, taking, weighing, returned_ref, out_ref, *, width):
    picked = matmul(taking[...], returned_ref[...])
    lanes = weighing.shape[1]
    weight = jnp.concatenate([weighing[...]] * (width // lanes), axis=1)
    weighted = picked * weight
    count, model = tokens_ref.shape
    rows = PIECES * count
    mixture = weighted[:rows]
    for k in range(1, weighted.shape[0] // rows):
        mixture = mixture + weighted[k * rows : (k + 1) * rows]
    for s in range(PIECES):
        span = min((s + 1) * width, model) - s * width
        here = pl.ds(s * width, span)
        out_ref[:, here] = (
            tokens_ref[:, here].astype(F32) + mixture[s * count : (s + 1) * count, :span]
        ).astype(BF16)


VMEM = pl.BlockSpec(memory_space=pltpu.VMEM)
MIB = 1 << 20


def call(kernel, out_shape, args, *, name, mib, flops):
    many = isinstance(out_shape, tuple)
    return pl.pallas_call(
        kernel,
        out_shape=out_shape,
        in_specs=[VMEM] * len(args),
        out_specs=(VMEM,) * len(out_shape) if many else VMEM,
        compiler_params=pltpu.CompilerParams(vmem_limit_bytes=mib * MIB),
        cost_estimate=pl.CostEstimate(flops=flops, bytes_accessed=0, transcendentals=0),
        name=name,
    )(*args)


def shards(tokens, norm_gain, expert_ids, gate_codes, w_gate, w_up, w_down):
    devices = lax.axis_size("ep")
    experts = devices // 2
    count, model = tokens.shape
    top = expert_ids.shape[1]
    width = piece_width(model)
    slots = experts * PIECES
    message = jax.ShapeDtypeStruct((slots, width), BF16)
    rows = jax.ShapeDtypeStruct((experts, model), BF16)
    same_core = [[2 * i + c for i in range(experts)] for c in range(2)]
    partner = [(i, i ^ 1) for i in range(devices)]
    ids = expert_ids.T
    codes = gate_codes.T
    picks = top * PIECES * count

    def exchange(array):
        return lax.all_to_all(
            array.reshape(experts, PIECES, width),
            "ep",
            split_axis=0,
            concat_axis=0,
            axis_index_groups=same_core,
            tiled=True,
        ).reshape(slots, width)

    spread = call(
        spread_kernel,
        jax.ShapeDtypeStruct((count, PIECES * count), BF16),
        (),
        name="spread",
        mib=1,
        flops=5_000_000_000,
    )
    outgoing = call(
        functools.partial(route_kernel, experts=experts, width=width),
        message,
        (tokens, norm_gain, ids, spread),
        name="route",
        mib=4,
        flops=20_000_000_000,
    )
    arrived = exchange(outgoing)
    other = lax.ppermute(arrived, "ep", partner)
    own_rows, taking, weighing = call(
        functools.partial(tables_kernel, model=model),
        (
            rows,
            jax.ShapeDtypeStruct((picks, slots), BF16),
            jax.ShapeDtypeStruct((picks, 128), F32),
        ),
        (arrived, ids, codes),
        name="tables",
        mib=8,
        flops=1_000_000_000,
    )
    own_share, other_share = call(
        expert_kernel,
        (rows, rows),
        (own_rows, other, w_gate[0].T, w_up[0].T, w_down[0]),
        name="expert",
        mib=32,
        flops=2_000_000_000,
    )
    arrived_share = lax.ppermute(other_share, "ep", partner)
    own_messages = call(
        functools.partial(messages_kernel, width=width),
        message,
        (own_share,),
        name="messages",
        mib=8,
        flops=1_000_000_000,
    )
    summed = call(
        functools.partial(add_kernel, width=width),
        message,
        (own_messages, arrived_share),
        name="add",
        mib=8,
        flops=1_000_000,
    )
    return call(
        functools.partial(combine_kernel, width=width),
        jax.ShapeDtypeStruct((count, model), BF16),
        (tokens, taking, weighing, exchange(summed)),
        name="combine",
        mib=8,
        flops=1_000_000,
    )


def solution(mesh):
    return jax.shard_map(
        shards,
        mesh=mesh,
        in_specs=(
            P(("groups", "ep"), None),
            P(),
            P(("groups", "ep"), None),
            P(("groups", "ep"), None),
            P("ep", None, None),
            P("ep", None, None),
            P("ep", None, None),
        ),
        out_specs=P(("groups", "ep"), None),
        check_vma=False,
    )
```

```python
import functools

import jax
import jax.numpy as jnp
from jax import lax
from jax.experimental import pallas as pl
from jax.experimental.pallas import tpu as pltpu
from jax.sharding import PartitionSpec as P

epsilon = 1e-05
PIECES = 8
BLOCK = 32
NT = (((1,), (1,)), ((), ()))
F32 = jnp.float32
BF16 = jnp.bfloat16


def iota(shape, axis):
    return lax.broadcasted_iota(jnp.int32, shape, axis)


def onehot(mask):
    return jnp.where(mask, 1.0, 0.0).astype(BF16)


def matmul(a, b):
    return jnp.dot(a, b, preferred_element_type=F32)


def piece_width(model_width):
    return -(-model_width // (PIECES * 128)) * 128


def stack_pieces(rows, width):
    n, d = rows.shape
    parts = []
    for s in range(PIECES):
        part = rows[:, s * width : min((s + 1) * width, d)]
        if part.shape[1] < width:
            part = jnp.concatenate(
                [part, jnp.zeros((n, width - part.shape[1]), rows.dtype)], axis=1
            )
        parts.append(part)
    return jnp.concatenate(parts, axis=0)


def swap_matrix(outer, inner):
    total = outer * inner
    row = iota((total, total), 0)
    col = iota((total, total), 1)
    return onehot(col == (row % inner) * outer + row // inner)


def rows_of(messages_ref):
    size = BLOCK * PIECES
    swap = swap_matrix(PIECES, BLOCK)
    blocks = []
    for b in range(messages_ref.shape[0] // size):
        moved = matmul(swap, messages_ref[b * size : (b + 1) * size, :]).astype(BF16)
        blocks.append(
            jnp.concatenate([moved[s * BLOCK : (s + 1) * BLOCK] for s in range(PIECES)], axis=1)
        )
    return jnp.concatenate(blocks, axis=0)


def messages_block(rows, width):
    return matmul(swap_matrix(BLOCK, PIECES), stack_pieces(rows, width))


def spread_kernel(spread_ref):
    count, columns = spread_ref.shape
    spread_ref[...] = onehot(iota((count, columns), 1) % count == iota((count, columns), 0))


def route_kernel(tokens_ref, gain_ref, ids_ref, spread_ref, out_ref, *, experts, width):
    top, count = ids_ref.shape
    columns = PIECES * count
    piece = iota((top, columns), 1) // count
    row = iota((experts * PIECES, columns), 0)
    ids = ids_ref[...].astype(F32).astype(BF16)
    wanted = matmul(ids, spread_ref[...]).astype(jnp.int32) * PIECES + piece
    hit = row == wanted[0:1, :]
    for k in range(1, top):
        hit = jnp.logical_or(hit, row == wanted[k : k + 1, :])
    placing = onehot(hit)
    values = tokens_ref[...].astype(F32)
    scale = lax.rsqrt(jnp.mean(values * values, axis=1, keepdims=True) + epsilon)
    normed = values * scale * gain_ref[...].reshape(1, -1)
    stacked = stack_pieces(normed, width).astype(BF16)
    out_ref[...] = matmul(placing, stacked).astype(BF16)


def tables_kernel(arrived_ref, ids_ref, codes_ref, own_rows, taking, weighing, *, model):
    own_rows[...] = rows_of(arrived_ref)[:, :model]
    ids = ids_ref[...].T
    codes = codes_ref[...].astype(F32)
    weights = (codes / jnp.sum(codes, axis=0, keepdims=True)).T
    count, top = ids.shape
    rows = PIECES * count
    piece = iota((rows, 1), 0) // count
    col = iota((rows, taking.shape[1]), 1)
    for k in range(top):
        here = pl.ds(k * rows, rows)
        wanted = jnp.concatenate([ids[:, k : k + 1]] * PIECES, axis=0) * PIECES + piece
        taking[here, :] = onehot(col == wanted)
        weight = jnp.concatenate([weights[:, k : k + 1]] * PIECES, axis=0)
        weighing[here, :] = jnp.broadcast_to(weight, (rows, weighing.shape[1]))


def expert_kernel(own_rows, other_ref, gate_ref, up_ref, down_ref, own_hidden, other_out):
    rows, model = own_rows.shape
    x = jnp.concatenate([rows_of(other_ref)[:, :model], own_rows[...]], axis=0)
    gate = lax.dot_general(gate_ref[...], x, NT, preferred_element_type=F32)
    up = lax.dot_general(up_ref[...], x, NT, preferred_element_type=F32)
    hidden = (gate * jax.nn.sigmoid(gate) * up).T.astype(BF16)
    own_hidden[...] = hidden[rows:]
    other_out[...] = matmul(hidden[:rows], down_ref[...]).astype(BF16)


def own_kernel(hidden_ref, down_ref, out_ref, *, width):
    size = BLOCK * PIECES
    share = matmul(hidden_ref[...], down_ref[...]).astype(BF16)
    for b in range(share.shape[0] // BLOCK):
        rows = share[b * BLOCK : (b + 1) * BLOCK]
        out_ref[b * size : (b + 1) * size, :] = messages_block(rows, width).astype(BF16)


def add_kernel(own_ref, arrived_ref, out_ref, *, width):
    size = BLOCK * PIECES
    for b in range(arrived_ref.shape[0] // BLOCK):
        here = pl.ds(b * size, size)
        moved = messages_block(arrived_ref[b * BLOCK : (b + 1) * BLOCK, :], width)
        out_ref[here, :] = (own_ref[here, :].astype(F32) + moved).astype(BF16)


def combine_kernel(tokens_ref, taking, weighing, returned_ref, out_ref, *, width):
    picked = matmul(taking[...], returned_ref[...])
    lanes = weighing.shape[1]
    weight = jnp.concatenate([weighing[...]] * (width // lanes), axis=1)
    weighted = picked * weight
    count, model = tokens_ref.shape
    rows = PIECES * count
    mixture = weighted[:rows]
    for k in range(1, weighted.shape[0] // rows):
        mixture = mixture + weighted[k * rows : (k + 1) * rows]
    for s in range(PIECES):
        span = min((s + 1) * width, model) - s * width
        here = pl.ds(s * width, span)
        out_ref[:, here] = (
            tokens_ref[:, here].astype(F32) + mixture[s * count : (s + 1) * count, :span]
        ).astype(BF16)


VMEM = pl.BlockSpec(memory_space=pltpu.VMEM)
MIB = 1 << 20


def call(kernel, out_shape, args, *, name, mib, flops):
    many = isinstance(out_shape, tuple)
    return pl.pallas_call(
        kernel,
        out_shape=out_shape,
        in_specs=[VMEM] * len(args),
        out_specs=(VMEM,) * len(out_shape) if many else VMEM,
        compiler_params=pltpu.CompilerParams(vmem_limit_bytes=mib * MIB),
        cost_estimate=pl.CostEstimate(flops=flops, bytes_accessed=0, transcendentals=0),
        name=name,
    )(*args)


def shards(tokens, norm_gain, expert_ids, gate_codes, w_gate, w_up, w_down):
    devices = lax.axis_size("ep")
    experts = devices // 2
    count, model = tokens.shape
    top = expert_ids.shape[1]
    width = piece_width(model)
    slots = experts * PIECES
    message = jax.ShapeDtypeStruct((slots, width), BF16)
    rows = jax.ShapeDtypeStruct((experts, model), BF16)
    same_core = [[2 * i + c for i in range(experts)] for c in range(2)]
    partner = [(i, i ^ 1) for i in range(devices)]
    ids = expert_ids.T
    codes = gate_codes.T
    picks = top * PIECES * count

    def exchange(array):
        return lax.all_to_all(
            array.reshape(experts, PIECES, width),
            "ep",
            split_axis=0,
            concat_axis=0,
            axis_index_groups=same_core,
            tiled=True,
        ).reshape(slots, width)

    spread = call(
        spread_kernel,
        jax.ShapeDtypeStruct((count, PIECES * count), BF16),
        (),
        name="spread",
        mib=1,
        flops=5_000_000_000,
    )
    outgoing = call(
        functools.partial(route_kernel, experts=experts, width=width),
        message,
        (tokens, norm_gain, ids, spread),
        name="route",
        mib=4,
        flops=20_000_000_000,
    )
    arrived = exchange(outgoing)
    other = lax.ppermute(arrived, "ep", partner)
    own_rows, taking, weighing = call(
        functools.partial(tables_kernel, model=model),
        (
            rows,
            jax.ShapeDtypeStruct((picks, slots), BF16),
            jax.ShapeDtypeStruct((picks, 128), F32),
        ),
        (arrived, ids, codes),
        name="tables",
        mib=8,
        flops=1_000_000_000,
    )
    own_hidden, other_share = call(
        expert_kernel,
        (jax.ShapeDtypeStruct((experts, w_down.shape[1]), BF16), rows),
        (own_rows, other, w_gate[0].T, w_up[0].T, w_down[0]),
        name="expert",
        mib=32,
        flops=2_000_000_000,
    )
    arrived_share = lax.ppermute(other_share, "ep", partner)
    own_messages = call(
        functools.partial(own_kernel, width=width),
        message,
        (own_hidden, w_down[0]),
        name="own",
        mib=16,
        flops=1_000_000_000,
    )
    summed = call(
        functools.partial(add_kernel, width=width),
        message,
        (own_messages, arrived_share),
        name="add",
        mib=8,
        flops=1_000_000,
    )
    return call(
        functools.partial(combine_kernel, width=width),
        jax.ShapeDtypeStruct((count, model), BF16),
        (tokens, taking, weighing, exchange(summed)),
        name="combine",
        mib=8,
        flops=1_000_000,
    )


def solution(mesh):
    return jax.shard_map(
        shards,
        mesh=mesh,
        in_specs=(
            P(("groups", "ep"), None),
            P(),
            P(("groups", "ep"), None),
            P(("groups", "ep"), None),
            P("ep", None, None),
            P("ep", None, None),
            P("ep", None, None),
        ),
        out_specs=P(("groups", "ep"), None),
        check_vma=False,
    )
```

```python
import functools
import math

import jax
import jax.numpy as jnp
from jax import lax
from jax.experimental import pallas as pl
from jax.experimental.pallas import tpu as pltpu
from jax.sharding import PartitionSpec as P

epsilon = 1e-05
PIECES = 8
BLOCK = 32
NT = (((1,), (1,)), ((), ()))
F32 = jnp.float32
BF16 = jnp.bfloat16


def iota(shape, axis):
    return lax.broadcasted_iota(jnp.int32, shape, axis)


def onehot(mask):
    return jnp.where(mask, 1.0, 0.0).astype(BF16)


def matmul(a, b):
    return jnp.dot(a, b, preferred_element_type=F32)


def place(expert, experts):
    side = math.isqrt(experts)
    half = side // 2
    row, column = expert // side, expert % side
    return (row + half * (column // half)) % side * side + column


def piece_width(model_width):
    return -(-model_width // (PIECES * 128)) * 128


def stack_pieces(rows, width):
    n, d = rows.shape
    parts = []
    for s in range(PIECES):
        part = rows[:, s * width : min((s + 1) * width, d)]
        if part.shape[1] < width:
            part = jnp.concatenate(
                [part, jnp.zeros((n, width - part.shape[1]), rows.dtype)], axis=1
            )
        parts.append(part)
    return jnp.concatenate(parts, axis=0)


def swap_matrix(outer, inner):
    total = outer * inner
    row = iota((total, total), 0)
    col = iota((total, total), 1)
    return onehot(col == (row % inner) * outer + row // inner)


def rows_of(messages_ref):
    size = BLOCK * PIECES
    swap = swap_matrix(PIECES, BLOCK)
    blocks = []
    for b in range(messages_ref.shape[0] // size):
        moved = matmul(swap, messages_ref[b * size : (b + 1) * size, :]).astype(BF16)
        blocks.append(
            jnp.concatenate([moved[s * BLOCK : (s + 1) * BLOCK] for s in range(PIECES)], axis=1)
        )
    return jnp.concatenate(blocks, axis=0)


def messages_block(rows, width):
    return matmul(swap_matrix(BLOCK, PIECES), stack_pieces(rows, width))


def spread_kernel(spread_ref):
    count, columns = spread_ref.shape
    spread_ref[...] = onehot(iota((count, columns), 1) % count == iota((count, columns), 0))


def route_kernel(tokens_ref, gain_ref, ids_ref, spread_ref, out_ref, *, experts, width):
    top, count = ids_ref.shape
    columns = PIECES * count
    piece = iota((top, columns), 1) // count
    row = iota((experts * PIECES, columns), 0)
    ids = ids_ref[...].astype(F32).astype(BF16)
    wanted = place(matmul(ids, spread_ref[...]).astype(jnp.int32), experts) * PIECES + piece
    hit = row == wanted[0:1, :]
    for k in range(1, top):
        hit = jnp.logical_or(hit, row == wanted[k : k + 1, :])
    placing = onehot(hit)
    values = tokens_ref[...].astype(F32)
    scale = lax.rsqrt(jnp.mean(values * values, axis=1, keepdims=True) + epsilon)
    normed = values * scale * gain_ref[...].reshape(1, -1)
    stacked = stack_pieces(normed, width).astype(BF16)
    out_ref[...] = matmul(placing, stacked).astype(BF16)


def tables_kernel(arrived_ref, ids_ref, codes_ref, own_rows, taking, weighing, *, model):
    own_rows[...] = rows_of(arrived_ref)[:, :model]
    ids = place(ids_ref[...], taking.shape[1] // PIECES).T
    codes = codes_ref[...].astype(F32)
    weights = (codes / jnp.sum(codes, axis=0, keepdims=True)).T
    count, top = ids.shape
    rows = PIECES * count
    piece = iota((rows, 1), 0) // count
    col = iota((rows, taking.shape[1]), 1)
    for k in range(top):
        here = pl.ds(k * rows, rows)
        wanted = jnp.concatenate([ids[:, k : k + 1]] * PIECES, axis=0) * PIECES + piece
        taking[here, :] = onehot(col == wanted)
        weight = jnp.concatenate([weights[:, k : k + 1]] * PIECES, axis=0)
        weighing[here, :] = jnp.broadcast_to(weight, (rows, weighing.shape[1]))


def expert_kernel(own_rows, other_ref, gate_ref, up_ref, down_ref, own_out, other_out):
    rows, model = own_rows.shape
    x = jnp.concatenate([own_rows[...], rows_of(other_ref)[:, :model]], axis=0)
    gate = lax.dot_general(gate_ref[...], x, NT, preferred_element_type=F32)
    up = lax.dot_general(up_ref[...], x, NT, preferred_element_type=F32)
    hidden = (gate * jax.nn.sigmoid(gate) * up).T.astype(BF16)
    out = matmul(hidden, down_ref[...]).astype(BF16)
    own_out[...] = out[:rows]
    other_out[...] = out[rows:]


def messages_kernel(rows_ref, out_ref, *, width):
    size = BLOCK * PIECES
    for b in range(rows_ref.shape[0] // BLOCK):
        rows = rows_ref[b * BLOCK : (b + 1) * BLOCK, :].astype(F32).astype(BF16)
        out_ref[b * size : (b + 1) * size, :] = messages_block(rows, width).astype(BF16)


def add_kernel(own_ref, arrived_ref, out_ref, *, width):
    size = BLOCK * PIECES
    for b in range(arrived_ref.shape[0] // BLOCK):
        here = pl.ds(b * size, size)
        moved = messages_block(arrived_ref[b * BLOCK : (b + 1) * BLOCK, :], width)
        out_ref[here, :] = (own_ref[here, :].astype(F32) + moved).astype(BF16)


def combine_kernel(tokens_ref, taking, weighing, returned_ref, out_ref, *, width):
    picked = matmul(taking[...], returned_ref[...])
    lanes = weighing.shape[1]
    weight = jnp.concatenate([weighing[...]] * (width // lanes), axis=1)
    weighted = picked * weight
    count, model = tokens_ref.shape
    rows = PIECES * count
    mixture = weighted[:rows]
    for k in range(1, weighted.shape[0] // rows):
        mixture = mixture + weighted[k * rows : (k + 1) * rows]
    for s in range(PIECES):
        span = min((s + 1) * width, model) - s * width
        here = pl.ds(s * width, span)
        out_ref[:, here] = (
            tokens_ref[:, here].astype(F32) + mixture[s * count : (s + 1) * count, :span]
        ).astype(BF16)


VMEM = pl.BlockSpec(memory_space=pltpu.VMEM)
MIB = 1 << 20


def call(kernel, out_shape, args, *, name, mib, flops):
    many = isinstance(out_shape, tuple)
    return pl.pallas_call(
        kernel,
        out_shape=out_shape,
        in_specs=[VMEM] * len(args),
        out_specs=(VMEM,) * len(out_shape) if many else VMEM,
        compiler_params=pltpu.CompilerParams(vmem_limit_bytes=mib * MIB),
        cost_estimate=pl.CostEstimate(flops=flops, bytes_accessed=0, transcendentals=0),
        name=name,
    )(*args)


def shards(tokens, norm_gain, expert_ids, gate_codes, w_gate, w_up, w_down):
    devices = lax.axis_size("ep")
    experts = devices // 2
    count, model = tokens.shape
    top = expert_ids.shape[1]
    width = piece_width(model)
    slots = experts * PIECES
    message = jax.ShapeDtypeStruct((slots, width), BF16)
    rows = jax.ShapeDtypeStruct((experts, model), BF16)
    same_core = [[2 * place(i, experts) + c for i in range(experts)] for c in range(2)]
    partner = [(i, i ^ 1) for i in range(devices)]
    ids = expert_ids.T
    codes = gate_codes.T
    picks = top * PIECES * count

    def exchange(array):
        return lax.all_to_all(
            array.reshape(experts, PIECES, width),
            "ep",
            split_axis=0,
            concat_axis=0,
            axis_index_groups=same_core,
            tiled=True,
        ).reshape(slots, width)

    spread = call(
        spread_kernel,
        jax.ShapeDtypeStruct((count, PIECES * count), BF16),
        (),
        name="spread",
        mib=1,
        flops=5_000_000_000,
    )
    outgoing = call(
        functools.partial(route_kernel, experts=experts, width=width),
        message,
        (tokens, norm_gain, ids, spread),
        name="route",
        mib=4,
        flops=20_000_000_000,
    )
    arrived = exchange(outgoing)
    other = lax.ppermute(arrived, "ep", partner)
    own_rows, taking, weighing = call(
        functools.partial(tables_kernel, model=model),
        (
            rows,
            jax.ShapeDtypeStruct((picks, slots), BF16),
            jax.ShapeDtypeStruct((picks, 128), F32),
        ),
        (arrived, ids, codes),
        name="tables",
        mib=8,
        flops=1_000_000_000,
    )
    own_share, other_share = call(
        expert_kernel,
        (rows, rows),
        (own_rows, other, w_gate[0].T, w_up[0].T, w_down[0]),
        name="expert",
        mib=32,
        flops=2_000_000_000,
    )
    arrived_share = lax.ppermute(other_share, "ep", partner)
    own_messages = call(
        functools.partial(messages_kernel, width=width),
        message,
        (own_share,),
        name="messages",
        mib=8,
        flops=1_000_000_000,
    )
    summed = call(
        functools.partial(add_kernel, width=width),
        message,
        (own_messages, arrived_share),
        name="add",
        mib=8,
        flops=1_000_000,
    )
    return call(
        functools.partial(combine_kernel, width=width),
        jax.ShapeDtypeStruct((count, model), BF16),
        (tokens, taking, weighing, exchange(summed)),
        name="combine",
        mib=8,
        flops=1_000_000,
    )


def solution(mesh):
    return jax.shard_map(
        shards,
        mesh=mesh,
        in_specs=(
            P(("groups", "ep"), None),
            P(),
            P(("groups", "ep"), None),
            P(("groups", "ep"), None),
            P("ep", None, None),
            P("ep", None, None),
            P("ep", None, None),
        ),
        out_specs=P(("groups", "ep"), None),
        check_vma=False,
    )
```

```python
import functools
import math

import jax
import jax.numpy as jnp
from jax import lax
from jax.experimental import pallas as pl
from jax.experimental.pallas import tpu as pltpu
from jax.sharding import PartitionSpec as P

epsilon = 1e-05
PIECES = 8
BLOCK = 16
NT = (((1,), (1,)), ((), ()))
F32 = jnp.float32
BF16 = jnp.bfloat16


def iota(shape, axis):
    return lax.broadcasted_iota(jnp.int32, shape, axis)


def onehot(mask):
    return jnp.where(mask, 1.0, 0.0).astype(BF16)


def matmul(a, b):
    return jnp.dot(a, b, preferred_element_type=F32)


def place(expert, experts):
    side = math.isqrt(experts)
    half = side // 2
    row, column = expert // side, expert % side
    return (row + half * (column // half)) % side * side + column


def piece_width(model_width):
    return -(-model_width // (PIECES * 128)) * 128


def stack_pieces(rows, width):
    n, d = rows.shape
    parts = []
    for s in range(PIECES):
        part = rows[:, s * width : min((s + 1) * width, d)]
        if part.shape[1] < width:
            part = jnp.concatenate(
                [part, jnp.zeros((n, width - part.shape[1]), rows.dtype)], axis=1
            )
        parts.append(part)
    return jnp.concatenate(parts, axis=0)


def swap_matrix(outer, inner):
    total = outer * inner
    row = iota((total, total), 0)
    col = iota((total, total), 1)
    return onehot(col == (row % inner) * outer + row // inner)


def rows_of(messages_ref):
    size = BLOCK * PIECES
    swap = swap_matrix(PIECES, BLOCK)
    blocks = []
    for b in range(messages_ref.shape[0] // size):
        moved = matmul(swap, messages_ref[b * size : (b + 1) * size, :]).astype(BF16)
        blocks.append(
            jnp.concatenate([moved[s * BLOCK : (s + 1) * BLOCK] for s in range(PIECES)], axis=1)
        )
    return jnp.concatenate(blocks, axis=0)


def messages_block(rows, width):
    return matmul(swap_matrix(BLOCK, PIECES), stack_pieces(rows, width))


def spread_kernel(spread_ref):
    count, columns = spread_ref.shape
    spread_ref[...] = onehot(iota((count, columns), 1) % count == iota((count, columns), 0))


def route_kernel(tokens_ref, gain_ref, ids_ref, spread_ref, out_ref, *, experts, width):
    top, count = ids_ref.shape
    columns = PIECES * count
    piece = iota((top, columns), 1) // count
    row = iota((experts * PIECES, columns), 0)
    ids = ids_ref[...].astype(F32).astype(BF16)
    wanted = place(matmul(ids, spread_ref[...]).astype(jnp.int32), experts) * PIECES + piece
    hit = row == wanted[0:1, :]
    for k in range(1, top):
        hit = jnp.logical_or(hit, row == wanted[k : k + 1, :])
    placing = onehot(hit)
    values = tokens_ref[...].astype(F32)
    scale = lax.rsqrt(jnp.mean(values * values, axis=1, keepdims=True) + epsilon)
    normed = values * scale * gain_ref[...].reshape(1, -1)
    stacked = stack_pieces(normed, width).astype(BF16)
    out_ref[...] = matmul(placing, stacked).astype(BF16)


def tables_kernel(arrived_ref, ids_ref, codes_ref, own_rows, taking, weighing, *, model):
    own_rows[...] = rows_of(arrived_ref)[:, :model]
    ids = place(ids_ref[...], taking.shape[1] // PIECES).T
    codes = codes_ref[...].astype(F32)
    weights = (codes / jnp.sum(codes, axis=0, keepdims=True)).T
    count, top = ids.shape
    rows = PIECES * count
    piece = iota((rows, 1), 0) // count
    col = iota((rows, taking.shape[1]), 1)
    for k in range(top):
        here = pl.ds(k * rows, rows)
        wanted = jnp.concatenate([ids[:, k : k + 1]] * PIECES, axis=0) * PIECES + piece
        taking[here, :] = onehot(col == wanted)
        weight = jnp.concatenate([weights[:, k : k + 1]] * PIECES, axis=0)
        weighing[here, :] = jnp.broadcast_to(weight, (rows, weighing.shape[1]))


def expert_kernel(own_rows, other_ref, gate_ref, up_ref, down_ref, own_out, other_out):
    rows, model = own_rows.shape
    x = jnp.concatenate([own_rows[...], rows_of(other_ref)[:, :model]], axis=0)
    gate = lax.dot_general(gate_ref[...], x, NT, preferred_element_type=F32)
    up = lax.dot_general(up_ref[...], x, NT, preferred_element_type=F32)
    hidden = (gate * jax.nn.sigmoid(gate) * up).T.astype(BF16)
    out = matmul(hidden, down_ref[...]).astype(BF16)
    own_out[...] = out[:rows]
    other_out[...] = out[rows:]


def messages_kernel(rows_ref, out_ref, *, width):
    size = BLOCK * PIECES
    for b in range(rows_ref.shape[0] // BLOCK):
        rows = rows_ref[b * BLOCK : (b + 1) * BLOCK, :]
        out_ref[b * size : (b + 1) * size, :] = messages_block(rows, width).astype(BF16)


def add_kernel(own_ref, arrived_ref, out_ref, *, width):
    size = BLOCK * PIECES
    for b in range(arrived_ref.shape[0] // BLOCK):
        here = pl.ds(b * size, size)
        moved = messages_block(arrived_ref[b * BLOCK : (b + 1) * BLOCK, :], width)
        out_ref[here, :] = (own_ref[here, :].astype(F32) + moved).astype(BF16)


def combine_kernel(tokens_ref, taking, weighing, returned_ref, out_ref, *, width):
    picked = matmul(taking[...], returned_ref[...])
    lanes = weighing.shape[1]
    weight = jnp.concatenate([weighing[...]] * (width // lanes), axis=1)
    weighted = picked * weight
    count, model = tokens_ref.shape
    rows = PIECES * count
    mixture = weighted[:rows]
    for k in range(1, weighted.shape[0] // rows):
        mixture = mixture + weighted[k * rows : (k + 1) * rows]
    for s in range(PIECES):
        span = min((s + 1) * width, model) - s * width
        here = pl.ds(s * width, span)
        out_ref[:, here] = (
            tokens_ref[:, here].astype(F32) + mixture[s * count : (s + 1) * count, :span]
        ).astype(BF16)


VMEM = pl.BlockSpec(memory_space=pltpu.VMEM)
MIB = 1 << 20


def call(kernel, out_shape, args, *, name, mib, flops):
    many = isinstance(out_shape, tuple)
    return pl.pallas_call(
        kernel,
        out_shape=out_shape,
        in_specs=[VMEM] * len(args),
        out_specs=(VMEM,) * len(out_shape) if many else VMEM,
        compiler_params=pltpu.CompilerParams(vmem_limit_bytes=mib * MIB),
        cost_estimate=pl.CostEstimate(flops=flops, bytes_accessed=0, transcendentals=0),
        name=name,
    )(*args)


def shards(tokens, norm_gain, expert_ids, gate_codes, w_gate, w_up, w_down):
    devices = lax.axis_size("ep")
    experts = devices // 2
    count, model = tokens.shape
    top = expert_ids.shape[1]
    width = piece_width(model)
    slots = experts * PIECES
    message = jax.ShapeDtypeStruct((slots, width), BF16)
    rows = jax.ShapeDtypeStruct((experts, model), BF16)
    same_core = [[2 * place(i, experts) + c for i in range(experts)] for c in range(2)]
    partner = [(i, i ^ 1) for i in range(devices)]
    ids = expert_ids.T
    codes = gate_codes.T
    picks = top * PIECES * count

    def exchange(array):
        return lax.all_to_all(
            array.reshape(experts, PIECES, width),
            "ep",
            split_axis=0,
            concat_axis=0,
            axis_index_groups=same_core,
            tiled=True,
        ).reshape(slots, width)

    spread = call(
        spread_kernel,
        jax.ShapeDtypeStruct((count, PIECES * count), BF16),
        (),
        name="spread",
        mib=1,
        flops=5_000_000_000,
    )
    outgoing = call(
        functools.partial(route_kernel, experts=experts, width=width),
        message,
        (tokens, norm_gain, ids, spread),
        name="route",
        mib=4,
        flops=20_000_000_000,
    )
    arrived = exchange(outgoing)
    other = lax.ppermute(arrived, "ep", partner)
    own_rows, taking, weighing = call(
        functools.partial(tables_kernel, model=model),
        (
            rows,
            jax.ShapeDtypeStruct((picks, slots), BF16),
            jax.ShapeDtypeStruct((picks, 128), F32),
        ),
        (arrived, ids, codes),
        name="tables",
        mib=8,
        flops=1_000_000_000,
    )
    own_share, other_share = call(
        expert_kernel,
        (rows, rows),
        (own_rows, other, w_gate[0].T, w_up[0].T, w_down[0]),
        name="expert",
        mib=32,
        flops=2_000_000_000,
    )
    arrived_share = lax.ppermute(other_share, "ep", partner)
    own_messages = call(
        functools.partial(messages_kernel, width=width),
        message,
        (own_share,),
        name="messages",
        mib=8,
        flops=1_000_000_000,
    )
    summed = call(
        functools.partial(add_kernel, width=width),
        message,
        (own_messages, arrived_share),
        name="add",
        mib=8,
        flops=1_000_000,
    )
    return call(
        functools.partial(combine_kernel, width=width),
        jax.ShapeDtypeStruct((count, model), BF16),
        (tokens, taking, weighing, exchange(summed)),
        name="combine",
        mib=8,
        flops=1_000_000,
    )


def solution(mesh):
    return jax.shard_map(
        shards,
        mesh=mesh,
        in_specs=(
            P(("groups", "ep"), None),
            P(),
            P(("groups", "ep"), None),
            P(("groups", "ep"), None),
            P("ep", None, None),
            P("ep", None, None),
            P("ep", None, None),
        ),
        out_specs=P(("groups", "ep"), None),
        check_vma=False,
    )
```

```python
import functools
import math

import jax
import jax.numpy as jnp
from jax import lax
from jax.experimental import pallas as pl
from jax.experimental.pallas import tpu as pltpu
from jax.sharding import PartitionSpec as P

epsilon = 1e-05
PIECES = 8
BLOCK = 16
NT = (((1,), (1,)), ((), ()))
F32 = jnp.float32
BF16 = jnp.bfloat16


def iota(shape, axis):
    return lax.broadcasted_iota(jnp.int32, shape, axis)


def onehot(mask):
    return jnp.where(mask, 1.0, 0.0).astype(BF16)


def matmul(a, b):
    return jnp.dot(a, b, preferred_element_type=F32)


def place(expert, experts):
    side = math.isqrt(experts)
    half = side // 2
    row, column = expert // side, expert % side
    return (row + half * (column // half)) % side * side + column


def piece_width(model_width):
    return -(-model_width // (PIECES * 128)) * 128


def stack_pieces(rows, width):
    n, d = rows.shape
    parts = []
    for s in range(PIECES):
        part = rows[:, s * width : min((s + 1) * width, d)]
        if part.shape[1] < width:
            part = jnp.concatenate(
                [part, jnp.zeros((n, width - part.shape[1]), rows.dtype)], axis=1
            )
        parts.append(part)
    return jnp.concatenate(parts, axis=0)


def swap_matrix(outer, inner):
    total = outer * inner
    row = iota((total, total), 0)
    col = iota((total, total), 1)
    return onehot(col == (row % inner) * outer + row // inner)


def rows_of(messages_ref):
    size = BLOCK * PIECES
    swap = swap_matrix(PIECES, BLOCK)
    blocks = []
    for b in range(messages_ref.shape[0] // size):
        moved = matmul(swap, messages_ref[b * size : (b + 1) * size, :]).astype(BF16)
        blocks.append(
            jnp.concatenate([moved[s * BLOCK : (s + 1) * BLOCK] for s in range(PIECES)], axis=1)
        )
    return jnp.concatenate(blocks, axis=0)


def messages_block(rows, width):
    return matmul(swap_matrix(BLOCK, PIECES), stack_pieces(rows, width))


def spread_kernel(spread_ref):
    count, columns = spread_ref.shape
    spread_ref[...] = onehot(iota((count, columns), 1) % count == iota((count, columns), 0))


def route_kernel(tokens_ref, gain_ref, ids_ref, spread_ref, out_ref, *, experts, width):
    top, count = ids_ref.shape
    columns = PIECES * count
    piece = iota((top, columns), 1) // count
    row = iota((experts * PIECES, columns), 0)
    ids = ids_ref[...].astype(F32).astype(BF16)
    wanted = place(matmul(ids, spread_ref[...]).astype(jnp.int32), experts) * PIECES + piece
    hit = row == wanted[0:1, :]
    for k in range(1, top):
        hit = jnp.logical_or(hit, row == wanted[k : k + 1, :])
    placing = onehot(hit)
    values = tokens_ref[...].astype(F32)
    scale = lax.rsqrt(jnp.mean(values * values, axis=1, keepdims=True) + epsilon)
    normed = values * scale * gain_ref[...].reshape(1, -1)
    stacked = stack_pieces(normed, width).astype(BF16)
    out_ref[...] = matmul(placing, stacked).astype(BF16)


def tables_kernel(arrived_ref, ids_ref, codes_ref, own_rows, taking, weighing, *, model):
    own_rows[...] = rows_of(arrived_ref)[:, :model]
    ids = place(ids_ref[...], taking.shape[1] // PIECES).T
    codes = codes_ref[...].astype(F32)
    weights = (codes / jnp.sum(codes, axis=0, keepdims=True)).T
    count, top = ids.shape
    rows = PIECES * count
    piece = iota((rows, 1), 0) // count
    col = iota((rows, taking.shape[1]), 1)
    for k in range(top):
        here = pl.ds(k * rows, rows)
        wanted = jnp.concatenate([ids[:, k : k + 1]] * PIECES, axis=0) * PIECES + piece
        taking[here, :] = onehot(col == wanted)
        weight = jnp.concatenate([weights[:, k : k + 1]] * PIECES, axis=0)
        weighing[here, :] = jnp.broadcast_to(weight, (rows, weighing.shape[1]))


def expert_kernel(own_rows, other_ref, gate_ref, up_ref, down_ref, own_out, other_out):
    rows, model = own_rows.shape
    x = jnp.concatenate([own_rows[...], rows_of(other_ref)[:, :model]], axis=0)
    cut = gate_ref.shape[0] // 256 * 128 + 128
    parts = []
    for low, high in ((0, cut), (cut, gate_ref.shape[0])):
        gate = lax.dot_general(gate_ref[low:high], x, NT, preferred_element_type=F32)
        up = lax.dot_general(up_ref[low:high], x, NT, preferred_element_type=F32)
        parts.append((gate * jax.nn.sigmoid(gate) * up).astype(BF16).T)
    hidden = jnp.concatenate(parts, axis=1)
    out = matmul(hidden, down_ref[...]).astype(BF16)
    own_out[...] = out[:rows]
    other_out[...] = out[rows:]


def messages_kernel(rows_ref, out_ref, *, width):
    size = BLOCK * PIECES
    for b in range(rows_ref.shape[0] // BLOCK):
        rows = rows_ref[b * BLOCK : (b + 1) * BLOCK, :]
        out_ref[b * size : (b + 1) * size, :] = messages_block(rows, width).astype(BF16)


def add_kernel(own_ref, arrived_ref, out_ref, *, width):
    size = BLOCK * PIECES
    for b in range(arrived_ref.shape[0] // BLOCK):
        here = pl.ds(b * size, size)
        moved = messages_block(arrived_ref[b * BLOCK : (b + 1) * BLOCK, :], width)
        out_ref[here, :] = (own_ref[here, :].astype(F32) + moved).astype(BF16)


def combine_kernel(tokens_ref, taking, weighing, returned_ref, out_ref, *, width):
    picked = matmul(taking[...], returned_ref[...])
    lanes = weighing.shape[1]
    weight = jnp.concatenate([weighing[...]] * (width // lanes), axis=1)
    weighted = picked * weight
    count, model = tokens_ref.shape
    rows = PIECES * count
    mixture = weighted[:rows]
    for k in range(1, weighted.shape[0] // rows):
        mixture = mixture + weighted[k * rows : (k + 1) * rows]
    for s in range(PIECES):
        span = min((s + 1) * width, model) - s * width
        here = pl.ds(s * width, span)
        out_ref[:, here] = (
            tokens_ref[:, here].astype(F32) + mixture[s * count : (s + 1) * count, :span]
        ).astype(BF16)


VMEM = pl.BlockSpec(memory_space=pltpu.VMEM)
MIB = 1 << 20


def call(kernel, out_shape, args, *, name, mib, flops):
    many = isinstance(out_shape, tuple)
    return pl.pallas_call(
        kernel,
        out_shape=out_shape,
        in_specs=[VMEM] * len(args),
        out_specs=(VMEM,) * len(out_shape) if many else VMEM,
        compiler_params=pltpu.CompilerParams(vmem_limit_bytes=mib * MIB),
        cost_estimate=pl.CostEstimate(flops=flops, bytes_accessed=0, transcendentals=0),
        name=name,
    )(*args)


def shards(tokens, norm_gain, expert_ids, gate_codes, w_gate, w_up, w_down):
    devices = lax.axis_size("ep")
    experts = devices // 2
    count, model = tokens.shape
    top = expert_ids.shape[1]
    width = piece_width(model)
    slots = experts * PIECES
    message = jax.ShapeDtypeStruct((slots, width), BF16)
    rows = jax.ShapeDtypeStruct((experts, model), BF16)
    same_core = [[2 * place(i, experts) + c for i in range(experts)] for c in range(2)]
    partner = [(i, i ^ 1) for i in range(devices)]
    ids = expert_ids.T
    codes = gate_codes.T
    picks = top * PIECES * count

    def exchange(array):
        return lax.all_to_all(
            array.reshape(experts, PIECES, width),
            "ep",
            split_axis=0,
            concat_axis=0,
            axis_index_groups=same_core,
            tiled=True,
        ).reshape(slots, width)

    spread = call(
        spread_kernel,
        jax.ShapeDtypeStruct((count, PIECES * count), BF16),
        (),
        name="spread",
        mib=1,
        flops=5_000_000_000,
    )
    outgoing = call(
        functools.partial(route_kernel, experts=experts, width=width),
        message,
        (tokens, norm_gain, ids, spread),
        name="route",
        mib=4,
        flops=20_000_000_000,
    )
    arrived = exchange(outgoing)
    other = lax.ppermute(arrived, "ep", partner)
    own_rows, taking, weighing = call(
        functools.partial(tables_kernel, model=model),
        (
            rows,
            jax.ShapeDtypeStruct((picks, slots), BF16),
            jax.ShapeDtypeStruct((picks, 128), F32),
        ),
        (arrived, ids, codes),
        name="tables",
        mib=8,
        flops=1_000_000_000,
    )
    own_share, other_share = call(
        expert_kernel,
        (rows, rows),
        (own_rows, other, w_gate[0].T, w_up[0].T, w_down[0]),
        name="expert",
        mib=32,
        flops=2_000_000_000,
    )
    arrived_share = lax.ppermute(other_share, "ep", partner)
    own_messages = call(
        functools.partial(messages_kernel, width=width),
        message,
        (own_share,),
        name="messages",
        mib=8,
        flops=1_000_000_000,
    )
    summed = call(
        functools.partial(add_kernel, width=width),
        message,
        (own_messages, arrived_share),
        name="add",
        mib=8,
        flops=1_000_000,
    )
    return call(
        functools.partial(combine_kernel, width=width),
        jax.ShapeDtypeStruct((count, model), BF16),
        (tokens, taking, weighing, exchange(summed)),
        name="combine",
        mib=8,
        flops=1_000_000,
    )


def solution(mesh):
    return jax.shard_map(
        shards,
        mesh=mesh,
        in_specs=(
            P(("groups", "ep"), None),
            P(),
            P(("groups", "ep"), None),
            P(("groups", "ep"), None),
            P("ep", None, None),
            P("ep", None, None),
            P("ep", None, None),
        ),
        out_specs=P(("groups", "ep"), None),
        check_vma=False,
    )
```

```python
import functools
import math

import jax
import jax.numpy as jnp
from jax import lax
from jax.experimental import pallas as pl
from jax.experimental.pallas import tpu as pltpu
from jax.sharding import PartitionSpec as P

epsilon = 1e-05
PIECES = 8
BLOCK = 16
NT = (((1,), (1,)), ((), ()))
F32 = jnp.float32
BF16 = jnp.bfloat16


def iota(shape, axis):
    return lax.broadcasted_iota(jnp.int32, shape, axis)


def onehot(mask):
    return jnp.where(mask, 1.0, 0.0).astype(BF16)


def matmul(a, b):
    return jnp.dot(a, b, preferred_element_type=F32)


def place(expert, experts):
    side = math.isqrt(experts)
    half = side // 2
    row, column = expert // side, expert % side
    return (row + half * (column // half)) % side * side + column


def piece_width(model_width):
    return -(-model_width // (PIECES * 128)) * 128


def stack_pieces(rows, width):
    n, d = rows.shape
    parts = []
    for s in range(PIECES):
        part = rows[:, s * width : min((s + 1) * width, d)]
        if part.shape[1] < width:
            part = jnp.concatenate(
                [part, jnp.zeros((n, width - part.shape[1]), rows.dtype)], axis=1
            )
        parts.append(part)
    return jnp.concatenate(parts, axis=0)


def swap_matrix(outer, inner):
    total = outer * inner
    row = iota((total, total), 0)
    col = iota((total, total), 1)
    return onehot(col == (row % inner) * outer + row // inner)


def rows_of(messages_ref):
    size = BLOCK * PIECES
    swap = swap_matrix(PIECES, BLOCK)
    blocks = []
    for b in range(messages_ref.shape[0] // size):
        moved = matmul(swap, messages_ref[b * size : (b + 1) * size, :]).astype(BF16)
        blocks.append(
            jnp.concatenate([moved[s * BLOCK : (s + 1) * BLOCK] for s in range(PIECES)], axis=1)
        )
    return jnp.concatenate(blocks, axis=0)


def messages_block(rows, width):
    return matmul(swap_matrix(BLOCK, PIECES), stack_pieces(rows, width))


def spread_kernel(spread_ref):
    count, columns = spread_ref.shape
    spread_ref[...] = onehot(iota((count, columns), 1) % count == iota((count, columns), 0))


def route_kernel(tokens_ref, gain_ref, ids_ref, spread_ref, out_ref, *, experts, width):
    top, count = ids_ref.shape
    columns = PIECES * count
    piece = iota((top, columns), 1) // count
    row = iota((experts * PIECES, columns), 0)
    ids = ids_ref[...].astype(F32).astype(BF16)
    wanted = place(matmul(ids, spread_ref[...]).astype(jnp.int32), experts) * PIECES + piece
    hit = row == wanted[0:1, :]
    for k in range(1, top):
        hit = jnp.logical_or(hit, row == wanted[k : k + 1, :])
    placing = onehot(hit)
    values = tokens_ref[...].astype(F32)
    scale = lax.rsqrt(jnp.mean(values * values, axis=1, keepdims=True) + epsilon)
    normed = values * scale * gain_ref[...].reshape(1, -1)
    stacked = stack_pieces(normed, width).astype(BF16)
    out_ref[...] = matmul(placing, stacked).astype(BF16)


def tables_kernel(arrived_ref, ids_ref, codes_ref, own_rows, taking, weighing, *, model):
    own_rows[...] = rows_of(arrived_ref)[:, :model]
    ids = place(ids_ref[...], taking.shape[1] // PIECES).T
    codes = codes_ref[...].astype(F32)
    weights = (codes / jnp.sum(codes, axis=0, keepdims=True)).T
    count, top = ids.shape
    rows = PIECES * count
    piece = iota((rows, 1), 0) // count
    col = iota((rows, taking.shape[1]), 1)
    for k in range(top):
        here = pl.ds(k * rows, rows)
        wanted = jnp.concatenate([ids[:, k : k + 1]] * PIECES, axis=0) * PIECES + piece
        taking[here, :] = onehot(col == wanted)
        weight = jnp.concatenate([weights[:, k : k + 1]] * PIECES, axis=0)
        weighing[here, :] = jnp.broadcast_to(weight, (rows, weighing.shape[1]))


def expert_kernel(own_rows, other_ref, gate_ref, up_ref, down_ref, own_out, other_out):
    rows, model = own_rows.shape
    x = jnp.concatenate([own_rows[...], rows_of(other_ref)[:, :model]], axis=0)
    units = gate_ref.shape[0]
    parts = []
    for low in range(0, units, 256):
        high = min(low + 256, units)
        gate = lax.dot_general(gate_ref[low:high], x, NT, preferred_element_type=F32)
        up = lax.dot_general(up_ref[low:high], x, NT, preferred_element_type=F32)
        parts.append((gate * jax.nn.sigmoid(gate) * up).astype(BF16).T)
    hidden = jnp.concatenate(parts, axis=1)
    out = matmul(hidden, down_ref[...]).astype(BF16)
    own_out[...] = out[:rows]
    other_out[...] = out[rows:]


def messages_kernel(rows_ref, out_ref, *, width):
    size = BLOCK * PIECES
    for b in range(rows_ref.shape[0] // BLOCK):
        rows = rows_ref[b * BLOCK : (b + 1) * BLOCK, :]
        out_ref[b * size : (b + 1) * size, :] = messages_block(rows, width).astype(BF16)


def add_kernel(own_ref, arrived_ref, out_ref, *, width):
    size = BLOCK * PIECES
    for b in range(arrived_ref.shape[0] // BLOCK):
        here = pl.ds(b * size, size)
        moved = messages_block(arrived_ref[b * BLOCK : (b + 1) * BLOCK, :], width)
        out_ref[here, :] = (own_ref[here, :].astype(F32) + moved).astype(BF16)


def combine_kernel(tokens_ref, taking, weighing, returned_ref, out_ref, *, width):
    picked = matmul(taking[...], returned_ref[...])
    lanes = weighing.shape[1]
    weight = jnp.concatenate([weighing[...]] * (width // lanes), axis=1)
    weighted = picked * weight
    count, model = tokens_ref.shape
    rows = PIECES * count
    mixture = weighted[:rows]
    for k in range(1, weighted.shape[0] // rows):
        mixture = mixture + weighted[k * rows : (k + 1) * rows]
    for s in range(PIECES):
        span = min((s + 1) * width, model) - s * width
        here = pl.ds(s * width, span)
        out_ref[:, here] = (
            tokens_ref[:, here].astype(F32) + mixture[s * count : (s + 1) * count, :span]
        ).astype(BF16)


VMEM = pl.BlockSpec(memory_space=pltpu.VMEM)
MIB = 1 << 20


def call(kernel, out_shape, args, *, name, mib, flops):
    many = isinstance(out_shape, tuple)
    return pl.pallas_call(
        kernel,
        out_shape=out_shape,
        in_specs=[VMEM] * len(args),
        out_specs=(VMEM,) * len(out_shape) if many else VMEM,
        compiler_params=pltpu.CompilerParams(vmem_limit_bytes=mib * MIB),
        cost_estimate=pl.CostEstimate(flops=flops, bytes_accessed=0, transcendentals=0),
        name=name,
    )(*args)


def shards(tokens, norm_gain, expert_ids, gate_codes, w_gate, w_up, w_down):
    devices = lax.axis_size("ep")
    experts = devices // 2
    count, model = tokens.shape
    top = expert_ids.shape[1]
    width = piece_width(model)
    slots = experts * PIECES
    message = jax.ShapeDtypeStruct((slots, width), BF16)
    rows = jax.ShapeDtypeStruct((experts, model), BF16)
    same_core = [[2 * place(i, experts) + c for i in range(experts)] for c in range(2)]
    partner = [(i, i ^ 1) for i in range(devices)]
    ids = expert_ids.T
    codes = gate_codes.T
    picks = top * PIECES * count

    def exchange(array):
        return lax.all_to_all(
            array.reshape(experts, PIECES, width),
            "ep",
            split_axis=0,
            concat_axis=0,
            axis_index_groups=same_core,
            tiled=True,
        ).reshape(slots, width)

    spread = call(
        spread_kernel,
        jax.ShapeDtypeStruct((count, PIECES * count), BF16),
        (),
        name="spread",
        mib=1,
        flops=5_000_000_000,
    )
    outgoing = call(
        functools.partial(route_kernel, experts=experts, width=width),
        message,
        (tokens, norm_gain, ids, spread),
        name="route",
        mib=4,
        flops=20_000_000_000,
    )
    arrived = exchange(outgoing)
    other = lax.ppermute(arrived, "ep", partner)
    own_rows, taking, weighing = call(
        functools.partial(tables_kernel, model=model),
        (
            rows,
            jax.ShapeDtypeStruct((picks, slots), BF16),
            jax.ShapeDtypeStruct((picks, 128), F32),
        ),
        (arrived, ids, codes),
        name="tables",
        mib=8,
        flops=1_000_000_000,
    )
    own_share, other_share = call(
        expert_kernel,
        (rows, rows),
        (own_rows, other, w_gate[0].T, w_up[0].T, w_down[0]),
        name="expert",
        mib=32,
        flops=2_000_000_000,
    )
    arrived_share = lax.ppermute(other_share, "ep", partner)
    own_messages = call(
        functools.partial(messages_kernel, width=width),
        message,
        (own_share,),
        name="messages",
        mib=8,
        flops=1_000_000_000,
    )
    summed = call(
        functools.partial(add_kernel, width=width),
        message,
        (own_messages, arrived_share),
        name="add",
        mib=8,
        flops=1_000_000,
    )
    return call(
        functools.partial(combine_kernel, width=width),
        jax.ShapeDtypeStruct((count, model), BF16),
        (tokens, taking, weighing, exchange(summed)),
        name="combine",
        mib=8,
        flops=1_000_000,
    )


def solution(mesh):
    return jax.shard_map(
        shards,
        mesh=mesh,
        in_specs=(
            P(("groups", "ep"), None),
            P(),
            P(("groups", "ep"), None),
            P(("groups", "ep"), None),
            P("ep", None, None),
            P("ep", None, None),
            P("ep", None, None),
        ),
        out_specs=P(("groups", "ep"), None),
        check_vma=False,
    )
```

```python
import functools
import math

import jax
import jax.numpy as jnp
from jax import lax
from jax.experimental import pallas as pl
from jax.experimental.pallas import tpu as pltpu
from jax.sharding import PartitionSpec as P

epsilon = 1e-05
PIECES = 8
BLOCK = 16
NT = (((1,), (1,)), ((), ()))
F32 = jnp.float32
BF16 = jnp.bfloat16


def iota(shape, axis):
    return lax.broadcasted_iota(jnp.int32, shape, axis)


def onehot(mask):
    return jnp.where(mask, 1.0, 0.0).astype(BF16)


def matmul(a, b):
    return jnp.dot(a, b, preferred_element_type=F32)


def place(expert, experts):
    side = math.isqrt(experts)
    half = side // 2
    row, column = expert // side, expert % side
    return (row + half * (column // half)) % side * side + column


def piece_width(model_width):
    return -(-model_width // (PIECES * 128)) * 128


def stack_pieces(rows, width):
    n, d = rows.shape
    parts = []
    for s in range(PIECES):
        part = rows[:, s * width : min((s + 1) * width, d)]
        if part.shape[1] < width:
            part = jnp.concatenate(
                [part, jnp.zeros((n, width - part.shape[1]), rows.dtype)], axis=1
            )
        parts.append(part)
    return jnp.concatenate(parts, axis=0)


def swap_matrix(outer, inner):
    total = outer * inner
    row = iota((total, total), 0)
    col = iota((total, total), 1)
    return onehot(col == (row % inner) * outer + row // inner)


def rows_of(messages_ref):
    size = BLOCK * PIECES
    swap = swap_matrix(PIECES, BLOCK)
    blocks = []
    for b in range(messages_ref.shape[0] // size):
        moved = matmul(swap, messages_ref[b * size : (b + 1) * size, :]).astype(BF16)
        blocks.append(
            jnp.concatenate([moved[s * BLOCK : (s + 1) * BLOCK] for s in range(PIECES)], axis=1)
        )
    return jnp.concatenate(blocks, axis=0)


def messages_block(rows, width):
    return matmul(swap_matrix(BLOCK, PIECES), stack_pieces(rows, width))


def slots_kernel(slots_ref, *, count):
    slots_ref[...] = iota(slots_ref.shape, 0) - iota(slots_ref.shape, 1) // count


def route_kernel(tokens_ref, gain_ref, ids_ref, slots_ref, out_ref, *, experts, width):
    top = ids_ref.shape[0]
    row = slots_ref[...]
    wanted = jnp.concatenate([place(ids_ref[...], experts) * PIECES] * PIECES, axis=1)
    hit = row == wanted[0:1, :]
    for k in range(1, top):
        hit = jnp.logical_or(hit, row == wanted[k : k + 1, :])
    placing = onehot(hit)
    values = tokens_ref[...].astype(F32)
    scale = lax.rsqrt(jnp.mean(values * values, axis=1, keepdims=True) + epsilon)
    normed = values * scale * gain_ref[...].reshape(1, -1)
    stacked = stack_pieces(normed, width).astype(BF16)
    out_ref[...] = matmul(placing, stacked).astype(BF16)


def tables_kernel(arrived_ref, ids_ref, codes_ref, own_rows, taking, weighing, *, model):
    own_rows[...] = rows_of(arrived_ref)[:, :model]
    ids = place(ids_ref[...], taking.shape[1] // PIECES).T
    codes = codes_ref[...].astype(F32)
    weights = (codes / jnp.sum(codes, axis=0, keepdims=True)).T
    count, top = ids.shape
    rows = PIECES * count
    piece = iota((rows, 1), 0) // count
    col = iota((rows, taking.shape[1]), 1)
    for k in range(top):
        here = pl.ds(k * rows, rows)
        wanted = jnp.concatenate([ids[:, k : k + 1]] * PIECES, axis=0) * PIECES + piece
        taking[here, :] = onehot(col == wanted)
        weight = jnp.concatenate([weights[:, k : k + 1]] * PIECES, axis=0)
        weighing[here, :] = jnp.broadcast_to(weight, (rows, weighing.shape[1]))


def expert_kernel(own_rows, other_ref, gate_ref, up_ref, down_ref, own_out, other_out):
    rows, model = own_rows.shape
    x = jnp.concatenate([own_rows[...], rows_of(other_ref)[:, :model]], axis=0)
    units = gate_ref.shape[0]
    parts = []
    for low in range(0, units, 256):
        high = min(low + 256, units)
        gate = lax.dot_general(gate_ref[low:high], x, NT, preferred_element_type=F32)
        up = lax.dot_general(up_ref[low:high], x, NT, preferred_element_type=F32)
        parts.append((gate * jax.nn.sigmoid(gate) * up).astype(BF16).T)
    hidden = jnp.concatenate(parts, axis=1)
    out = matmul(hidden, down_ref[...]).astype(BF16)
    own_out[...] = out[:rows]
    other_out[...] = out[rows:]


def messages_kernel(rows_ref, out_ref, *, width):
    size = BLOCK * PIECES
    for b in range(rows_ref.shape[0] // BLOCK):
        rows = rows_ref[b * BLOCK : (b + 1) * BLOCK, :]
        out_ref[b * size : (b + 1) * size, :] = messages_block(rows, width).astype(BF16)


def add_kernel(own_ref, arrived_ref, out_ref, *, width):
    size = BLOCK * PIECES
    for b in range(arrived_ref.shape[0] // BLOCK):
        here = pl.ds(b * size, size)
        moved = messages_block(arrived_ref[b * BLOCK : (b + 1) * BLOCK, :], width)
        out_ref[here, :] = (own_ref[here, :].astype(F32) + moved).astype(BF16)


def combine_kernel(tokens_ref, taking, weighing, returned_ref, out_ref, *, width):
    picked = matmul(taking[...], returned_ref[...])
    lanes = weighing.shape[1]
    weight = jnp.concatenate([weighing[...]] * (width // lanes), axis=1)
    weighted = picked * weight
    count, model = tokens_ref.shape
    rows = PIECES * count
    mixture = weighted[:rows]
    for k in range(1, weighted.shape[0] // rows):
        mixture = mixture + weighted[k * rows : (k + 1) * rows]
    for s in range(PIECES):
        span = min((s + 1) * width, model) - s * width
        here = pl.ds(s * width, span)
        out_ref[:, here] = (
            tokens_ref[:, here].astype(F32) + mixture[s * count : (s + 1) * count, :span]
        ).astype(BF16)


VMEM = pl.BlockSpec(memory_space=pltpu.VMEM)
MIB = 1 << 20


def call(kernel, out_shape, args, *, name, mib, flops):
    many = isinstance(out_shape, tuple)
    return pl.pallas_call(
        kernel,
        out_shape=out_shape,
        in_specs=[VMEM] * len(args),
        out_specs=(VMEM,) * len(out_shape) if many else VMEM,
        compiler_params=pltpu.CompilerParams(vmem_limit_bytes=mib * MIB),
        cost_estimate=pl.CostEstimate(flops=flops, bytes_accessed=0, transcendentals=0),
        name=name,
    )(*args)


def shards(tokens, norm_gain, expert_ids, gate_codes, w_gate, w_up, w_down):
    devices = lax.axis_size("ep")
    experts = devices // 2
    count, model = tokens.shape
    top = expert_ids.shape[1]
    width = piece_width(model)
    slots = experts * PIECES
    message = jax.ShapeDtypeStruct((slots, width), BF16)
    rows = jax.ShapeDtypeStruct((experts, model), BF16)
    same_core = [[2 * place(i, experts) + c for i in range(experts)] for c in range(2)]
    partner = [(i, i ^ 1) for i in range(devices)]
    ids = expert_ids.T
    codes = gate_codes.T
    picks = top * PIECES * count

    def exchange(array):
        return lax.all_to_all(
            array.reshape(experts, PIECES, width),
            "ep",
            split_axis=0,
            concat_axis=0,
            axis_index_groups=same_core,
            tiled=True,
        ).reshape(slots, width)

    table = call(
        functools.partial(slots_kernel, count=count),
        jax.ShapeDtypeStruct((slots, PIECES * count), jnp.int32),
        (),
        name="slots",
        mib=1,
        flops=5_000_000_000,
    )
    outgoing = call(
        functools.partial(route_kernel, experts=experts, width=width),
        message,
        (tokens, norm_gain, ids, table),
        name="route",
        mib=4,
        flops=20_000_000_000,
    )
    arrived = exchange(outgoing)
    other = lax.ppermute(arrived, "ep", partner)
    own_rows, taking, weighing = call(
        functools.partial(tables_kernel, model=model),
        (
            rows,
            jax.ShapeDtypeStruct((picks, slots), BF16),
            jax.ShapeDtypeStruct((picks, 128), F32),
        ),
        (arrived, ids, codes),
        name="tables",
        mib=8,
        flops=1_000_000_000,
    )
    own_share, other_share = call(
        expert_kernel,
        (rows, rows),
        (own_rows, other, w_gate[0].T, w_up[0].T, w_down[0]),
        name="expert",
        mib=32,
        flops=2_000_000_000,
    )
    arrived_share = lax.ppermute(other_share, "ep", partner)
    own_messages = call(
        functools.partial(messages_kernel, width=width),
        message,
        (own_share,),
        name="messages",
        mib=8,
        flops=1_000_000_000,
    )
    summed = call(
        functools.partial(add_kernel, width=width),
        message,
        (own_messages, arrived_share),
        name="add",
        mib=8,
        flops=1_000_000,
    )
    return call(
        functools.partial(combine_kernel, width=width),
        jax.ShapeDtypeStruct((count, model), BF16),
        (tokens, taking, weighing, exchange(summed)),
        name="combine",
        mib=8,
        flops=1_000_000,
    )


def solution(mesh):
    return jax.shard_map(
        shards,
        mesh=mesh,
        in_specs=(
            P(("groups", "ep"), None),
            P(),
            P(("groups", "ep"), None),
            P(("groups", "ep"), None),
            P("ep", None, None),
            P("ep", None, None),
            P("ep", None, None),
        ),
        out_specs=P(("groups", "ep"), None),
        check_vma=False,
    )
```
